32 devices in a mesh: pert: 2 (over x), ga: 16 (over z, y, core).
Axes of the slice: x: 2, y: 2, z: 4, core: 2. Of those that a mesh axis runs over, the one named last changes fastest.
Arguments:
- psi_k: bfloat16 [2, 8192, 256], P(None, 'ga'), may hold values from -6 to 6
- beta_k: bfloat16 [2, 8192, 2496], P(None, 'ga'), may hold values from -0.0625 to 0.0625
- beta_kq: bfloat16 [2, 8192, 2496], P(None, 'ga'), may hold values from -0.15625 to 0.15625
- g_k: float32 [3, 8192], P(None, 'ga'), may hold values from -2 to 2
- g_kq: float32 [3, 8192], P(None, 'ga'), may hold values from -2 to 2
- send_index: int32 [16, 16, 32], P('ga'), may hold values from -1 to 511, as said below
- recv_index: int32 [8192], P('ga'), may hold values from -1 to 511, as said below
- dmat: float32 [192, 13, 13], replicated, may hold values from -0.5 to 4, as said below
- displaced: int32 [256], P('pert'), parts along dimension 0, may hold values from 0 to 191, as said below
- mode: float32 [3, 256], P(None, 'pert'), parts along dimension 1, may hold values from -5 to 5
Outputs:
- dvpsi: bfloat16 [4, 8192, 256], P('pert', 'ga'), parts along dimension 0
The draws below stay inside these ranges and needn't reach their ends.
There are 2 independent parts, one for each index of `pert`. The reference program is written for one: setup_inputs(seed, part) draws one part's arguments, and reference() takes and returns one part's arrays. A program takes and returns all parts, laid end to end along the dimension named above; an argument that names none is the same for every part. Nothing has to cross between parts.
Inputs may be any that keep to these rules, and one draw needn't show every extreme that they name: `send_index`: entry [s, d, c] is a row of device s's k-sphere block in local numbering, or -1 for an unused slot; the rows device s sends are distinct; in every draw some device receives 32 rows from every device. `recv_index`: entry r is s * 32 + c, naming slot c from device s among the rows received by the device of row r, or -1 for a row with no k-sphere counterpart; every used slot is named by exactly one row of its receiving device and no unused slot is named. `dmat`: each atom's block is symmetric. `displaced`: 128 distinct atoms.
All inputs are finite; a program needn't handle non-finite values.
Results may differ from the reference program's by a relative error of at most 0.0057.
Values may be sent and summed in bfloat16 or wider, within the bound.
No kernel may reach another device: no remote copies, remote signals or barrier semaphores. Data moves between devices by JAX's collectives and lax.ppermute only.
A program may use at most 128 MiB of HBM per device.

```python
import jax
import jax.numpy as jnp
from jax import lax

KQ_DEV = 512
NB = 256
NPROJ_ATOM = 13
ATOMS = 192
DISP = 128
CAP = 32
NPW_Q = 8192
NPROJ = 2496
N_GA = 16


def exchange_plan(key):
    base = jax.random.fold_in(key, 7)
    key_counts, key_full, key_send, key_rows = jax.random.split(base, 4)
    short_draw = jax.random.randint(key_counts, (N_GA, N_GA), 0, 10)
    counts = jnp.where(short_draw == 0, CAP - 1, CAP)
    full_target = jax.random.randint(key_full, (), 0, N_GA)
    counts = jnp.where(jnp.arange(N_GA)[None, :] == full_target, CAP, counts).astype(jnp.int32)
    send_order = jax.vmap(lambda single: jax.random.permutation(single, KQ_DEV))(jax.random.split(key_send, N_GA)).astype(jnp.int32)
    slot_ids = jnp.arange(CAP, dtype=jnp.int32)
    offsets = jnp.cumsum(counts, axis=1) - counts
    positions = jnp.minimum(offsets[:, :, None] + slot_ids[None, None, :], KQ_DEV - 1).reshape(N_GA, N_GA * CAP)
    sent_rows = jnp.take_along_axis(send_order, positions, axis=1).reshape(N_GA, N_GA, CAP)
    live_slots = slot_ids[None, None, :] < counts[:, :, None]
    send_table = jnp.where(live_slots, sent_rows, -1).astype(jnp.int32)
    live_dest = jnp.transpose(live_slots, (1, 0, 2)).reshape(N_GA, N_GA * CAP)
    live_order = jnp.argsort(jnp.where(live_dest, 0, 1).astype(jnp.int32), axis=1, stable=True).astype(jnp.int32)
    live_total = jnp.sum(live_dest.astype(jnp.int32), axis=1)
    padded_order = jnp.concatenate([live_order, jnp.zeros((N_GA, KQ_DEV - N_GA * CAP), jnp.int32)], axis=1)
    row_ids = jnp.arange(KQ_DEV, dtype=jnp.int32)
    buffer_vals = jnp.where(row_ids[None, :] < live_total[:, None], padded_order, -1).astype(jnp.int32)
    row_perms = jax.vmap(lambda single: jax.random.permutation(single, KQ_DEV))(jax.random.split(key_rows, N_GA)).astype(jnp.int32)
    recv_table = jnp.zeros((N_GA, KQ_DEV), jnp.int32).at[jnp.arange(N_GA)[:, None], row_perms].set(buffer_vals)
    return (send_table, recv_table.reshape(-1))


def draw_send_index(key, part):
    send_table, recv_table = exchange_plan(key)
    return send_table


def draw_recv_index(key, part):
    send_table, recv_table = exchange_plan(key)
    return recv_table


def draw_dmat(key, part):
    key_off, key_diag = jax.random.split(jax.random.fold_in(key, 11))
    raw = jnp.clip(0.3 * jax.random.normal(key_off, (ATOMS, NPROJ_ATOM, NPROJ_ATOM), jnp.float32), -0.5, 0.5)
    symmetric = 0.5 * (raw + jnp.swapaxes(raw, 1, 2))
    diagonal = jax.random.uniform(key_diag, (ATOMS, NPROJ_ATOM), jnp.float32, 0.5, 2.5)
    identity = jnp.eye(NPROJ_ATOM, dtype=jnp.float32)
    return symmetric * (1.0 - identity) + diagonal[:, :, None] * identity


def draw_displaced(key, part):
    chosen = jax.random.permutation(jax.random.fold_in(key, 13), ATOMS)
    return chosen[:DISP].astype(jnp.int32)


def shard_levels(stream_key, shape, cuts, smallest, high):
    loudness = 1.0
    for dim, parts in cuts:
        steps = jax.random.uniform(jax.random.fold_in(jax.random.fold_in(stream_key, 6), dim), (parts,), jnp.float32, smallest / len(cuts), high / len(cuts))
        loudness = loudness * jnp.repeat(jnp.exp(steps), shape[dim] // parts).reshape((-1,) + (1,) * (len(shape) - 1 - dim))
    return loudness


def bell_draw(key, shape, deviation, most, cuts=(), kind=jnp.bfloat16):
    result = jax.random.normal(key, shape, jnp.float32) * deviation
    if len(cuts) > 0:
        result = shard_levels(key, shape, cuts, -0.22, 0.18) * result
    return jnp.clip(result, min=-most, max=most).astype(kind)


def setup_inputs(seed: int = 0, part: int = 0) -> dict:
    arg_keys = jax.random.split(jax.random.key(seed), 11)
    own_keys = jax.random.split(jax.random.fold_in(arg_keys[10], part), 11)
    psi_k = bell_draw(arg_keys[0], (2, NPW_Q, NB), 1.0, 6.0, ((1, 16),))
    beta_k = bell_draw(arg_keys[1], (2, NPW_Q, NPROJ), NPW_Q ** -0.5, 0.0625, ((1, 16),))
    beta_kq = bell_draw(arg_keys[2], (2, NPW_Q, NPROJ), (DISP * NPROJ_ATOM) ** -0.5, 0.15625, ((1, 16),))
    g_k = jnp.clip(jax.random.uniform(arg_keys[3], (3, NPW_Q), jnp.float32, -2.0, 2.0) * shard_levels(arg_keys[3], (3, NPW_Q), ((1, 16),), -0.4, 0.0), -2.0, 2.0)
    g_kq = jnp.clip(jax.random.uniform(arg_keys[4], (3, NPW_Q), jnp.float32, -2.0, 2.0) * shard_levels(arg_keys[4], (3, NPW_Q), ((1, 16),), -0.4, 0.0), -2.0, 2.0)
    send_index = draw_send_index(jax.random.fold_in(arg_keys[10], 71), part)
    recv_index = draw_recv_index(jax.random.fold_in(arg_keys[10], 71), part)
    dmat = draw_dmat(jax.random.fold_in(arg_keys[10], 71), part)
    displaced = draw_displaced(jax.random.fold_in(jax.random.fold_in(arg_keys[10], part), 71), part)
    mode = bell_draw(own_keys[9], (3, DISP), 1.0, 5.0, (), jnp.float32)
    return dict(psi_k=psi_k, beta_k=beta_k, beta_kq=beta_kq, g_k=g_k, g_kq=g_kq, send_index=send_index, recv_index=recv_index, dmat=dmat, displaced=displaced, mode=mode)


def contract_rows(left_side, stacked):
    return lax.dot_general(left_side, stacked, (((0,), (0,)), ((), ())), preferred_element_type=jnp.float32)


def local_terms(wave_rows, beta_rows, g_vectors, columns, weights):
    band_count = wave_rows.shape[2]
    picked = jnp.take(beta_rows, columns, axis=2)
    row_scale = jnp.dot(g_vectors.T, weights, precision=lax.Precision.HIGHEST, preferred_element_type=jnp.float32)
    conj_real = (row_scale * picked[1]).astype(jnp.bfloat16)
    conj_imag = (row_scale * picked[0]).astype(jnp.bfloat16)
    stacked = jnp.concatenate([wave_rows[0], wave_rows[1]], axis=1)
    with_real = contract_rows(picked[0], stacked)
    with_imag = contract_rows(picked[1], stacked)
    slope_real = contract_rows(conj_real, stacked)
    slope_imag = contract_rows(conj_imag, stacked)
    plain_part = jnp.stack([with_real[:, :band_count] + with_imag[:, band_count:],
                            with_real[:, band_count:] - with_imag[:, :band_count]])
    slope_part = jnp.stack([slope_real[:, :band_count] - slope_imag[:, band_count:],
                            slope_real[:, band_count:] + slope_imag[:, :band_count]])
    return jnp.stack([plain_part, slope_part])


def couple_atoms(summed, coupling):
    shape_in = summed.shape
    blocks = summed.reshape(2, 2, coupling.shape[0], coupling.shape[1], shape_in[3])
    mixed = jnp.einsum("dij,xcdjn->xcdin", coupling, blocks, precision=lax.Precision.HIGHEST)
    return mixed.reshape(shape_in).astype(jnp.bfloat16)


def back_project(coupled, beta_rows, g_vectors, columns, weights):
    band_count = coupled.shape[3]
    picked = jnp.take(beta_rows, columns, axis=2)
    row_scale = jnp.dot(g_vectors.T, weights, precision=lax.Precision.HIGHEST, preferred_element_type=jnp.float32)
    slope_real = (row_scale * picked[1]).astype(jnp.bfloat16)
    slope_imag = (-row_scale * picked[0]).astype(jnp.bfloat16)
    left_side = jnp.concatenate([slope_real, slope_imag, picked[0], picked[1]], axis=1)
    bra_terms = coupled[0]
    ket_terms = coupled[1]
    real_part = jnp.concatenate([bra_terms[0], -bra_terms[1], ket_terms[0], -ket_terms[1]], axis=0)
    imag_part = jnp.concatenate([bra_terms[1], bra_terms[0], ket_terms[1], ket_terms[0]], axis=0)
    right_side = jnp.concatenate([real_part, imag_part], axis=1)
    product = jnp.dot(left_side, right_side, preferred_element_type=jnp.float32)
    return jnp.stack([product[:, :band_count], product[:, band_count:]]).astype(jnp.bfloat16)


def reference(psi_k, beta_k, beta_kq, g_k, g_kq, send_index, recv_index, dmat, displaced, mode):
    row_total = recv_index.shape[0]
    row_ids = jnp.arange(row_total, dtype=jnp.int32)
    target = (row_ids // KQ_DEV).astype(jnp.int32)
    buffer_pos = jnp.maximum(recv_index, 0).astype(jnp.int32)
    source = (buffer_pos // CAP).astype(jnp.int32)
    slot_ids = (buffer_pos % CAP).astype(jnp.int32)
    local_row = send_index[source, target, slot_ids]
    live_rows = (recv_index >= 0) & (local_row >= 0)
    anchor = (source * KQ_DEV + jnp.maximum(local_row, 0)).astype(jnp.int32)
    psi_kq = jnp.where(live_rows[None, :, None], psi_k[:, anchor, :], jnp.zeros((), psi_k.dtype))
    columns = (displaced[:, None] * NPROJ_ATOM + jnp.arange(NPROJ_ATOM, dtype=jnp.int32)[None, :]).reshape(-1).astype(jnp.int32)
    atom_of = jnp.repeat(jnp.arange(DISP, dtype=jnp.int32), NPROJ_ATOM)
    weights = mode[:, atom_of]
    proj_count = columns.shape[0]

    def project_block(running, block_id):
        row_start = (block_id * KQ_DEV).astype(jnp.int32)
        wave_rows = lax.dynamic_slice_in_dim(psi_kq, row_start, KQ_DEV, 1)
        beta_rows = lax.dynamic_slice_in_dim(beta_k, row_start, KQ_DEV, 1)
        g_vectors = lax.dynamic_slice_in_dim(g_k, row_start, KQ_DEV, 1)
        return running + local_terms(wave_rows, beta_rows, g_vectors, columns, weights), None

    start_sum = jnp.zeros((2, 2, proj_count, NB), jnp.float32)
    summed, unused = lax.scan(project_block, start_sum, jnp.arange(N_GA, dtype=jnp.int32))
    coupling = jnp.take(dmat, displaced, axis=0)
    coupled = couple_atoms(summed, coupling)

    def apply_block(block_id):
        row_start = (block_id * KQ_DEV).astype(jnp.int32)
        beta_rows = lax.dynamic_slice_in_dim(beta_kq, row_start, KQ_DEV, 1)
        g_vectors = lax.dynamic_slice_in_dim(g_kq, row_start, KQ_DEV, 1)
        return back_project(coupled, beta_rows, g_vectors, columns, weights)

    pieces = lax.map(apply_block, jnp.arange(N_GA, dtype=jnp.int32))
    return jnp.transpose(pieces, (1, 0, 2, 3)).reshape(2, row_total, NB)
```

```python
import functools

import jax
import jax.numpy as jnp
import numpy as np
from jax import lax
from jax.experimental import pallas as pl
from jax.experimental.pallas import tpu as pltpu
from jax.sharding import PartitionSpec as P

F32, BF16 = jnp.float32, jnp.bfloat16
LANES = 128
SMEM = pl.BlockSpec(memory_space=pltpu.SMEM)


def stage_bits(count):
    first = list(range(count))
    second = list(first)
    if count > 2:
        second[1], second[2] = 2, 1
    return first, second


def block_order(bits):
    count = len(bits)
    return [
        sum(((place >> (count - 1 - i)) & 1) << bits[i] for i in range(count))
        for place in range(1 << count)
    ]


def cost(flops, moved):
    return pl.CostEstimate(flops=flops, bytes_accessed=moved, transcendentals=0)


def pack_kernel(slot_ref, psi_ref, out_ref):
    rows, slots = psi_ref.shape[1], slot_ref.shape[1]
    chosen = lax.broadcasted_iota(jnp.int32, (rows, slots), 0) == slot_ref[...]
    chosen = chosen.astype(BF16)
    bands = psi_ref.shape[2]
    for part in range(2):
        rows_out = lax.dot_general(
            chosen, psi_ref[part], (((0,), (0,)), ((), ())), preferred_element_type=F32
        )
        out_ref[:, part * bands : (part + 1) * bands] = rows_out.astype(BF16)


def pack_rows(slots, psi):
    count = slots.shape[1]
    return pl.pallas_call(
        pack_kernel,
        out_shape=jax.ShapeDtypeStruct((count, 2 * psi.shape[2]), BF16),
        cost_estimate=cost(2 * count * psi.shape[1] * 512, 2_000_000),
    )(slots, psi)


def place_kernel(recv_ref, out_ref):
    chosen = lax.broadcasted_iota(jnp.int32, out_ref.shape, 0) == recv_ref[...]
    out_ref[...] = chosen.astype(F32).T.astype(BF16)


def place_matrix(recv, slots):
    return pl.pallas_call(
        place_kernel, out_shape=jax.ShapeDtypeStruct((recv.shape[1], slots), BF16)
    )(recv)


def widen_rows(source, wide):
    rows, step = source.shape[1], 96
    while rows % step:
        step -= 8

    def body(index, carry):
        start = pl.multiple_of(index * step, 8)
        for l in range(wide.shape[0]):
            lanes = slice(LANES * l, LANES * (l + 1))
            wide[l, pl.ds(start, step), :] = source[0, pl.ds(start, step), lanes].astype(F32)
        return carry

    lax.fori_loop(0, rows // step, body, 0)


def walk_atoms(wide, tables, vectors, place, atoms, size, store):
    home, order, displaced, mode = tables
    base = (home[0] ^ order[place]) * atoms
    for i in range(atoms):
        start = displaced[base + i] * size
        amount = [mode[x, base + i] for x in range(3)]
        for l in range(wide.shape[0]):
            lanes = slice(LANES * l, LANES * (l + 1))
            picked = wide[l, pl.ds(start, size), :]
            weight = (
                amount[0] * vectors[0:1, lanes]
                + amount[1] * vectors[1:2, lanes]
                + amount[2] * vectors[2:3, lanes]
            )
            store(i, l, picked, weight)


def bra_kernel(atoms, size, home, order, swap, displaced, mode, source, vectors, *rest):
    plain, scaled, wide, slab, slab_scaled = rest[0:2], rest[2:4], rest[4], rest[5], rest[6]
    half, block = plain[0].shape[1:3]
    widen_rows(source, wide)
    if block != atoms * size:
        slab[...] = jnp.zeros_like(slab)
        slab_scaled[...] = jnp.zeros_like(slab_scaled)

    def store(i, l, picked, weight):
        slab[l, size * i : size * (i + 1), :] = picked
        slab_scaled[l, size * i : size * (i + 1), :] = picked * weight

    for h in range(2):

        def body(index, carry):
            place = h * half + index
            walk_atoms(
                wide, (home, order, displaced, mode), vectors, place, atoms, size, store
            )
            other = swap[place] - h * half
            for l in range(wide.shape[0]):
                lanes = slice(LANES * l, LANES * (l + 1))
                plain[h][0, index, :, lanes] = slab[l].astype(BF16)
                scaled[h][0, other, :, lanes] = slab_scaled[l].astype(BF16)
            return carry

        lax.fori_loop(0, half, body, 0)


def ket_kernel(atoms, size, block, home, order, swap, displaced, mode, source, vectors, *rest):
    turned, wide, slab = rest[0:2], rest[2], rest[3]
    half = slab.shape[1] // (2 * block)
    widen_rows(source, wide)
    if block != atoms * size:
        slab[...] = jnp.zeros_like(slab)
    for h in range(2):

        def body(index, carry):
            place = h * half + index
            plain_row = pl.multiple_of((swap[place] - h * half) * block, 8)
            scaled_row = pl.multiple_of((half + index) * block, 8)

            def store(i, l, picked, weight):
                slab[l, pl.ds(plain_row + size * i, size), :] = picked
                slab[l, pl.ds(scaled_row + size * i, size), :] = -(picked * weight)

            walk_atoms(
                wide, (home, order, displaced, mode), vectors, place, atoms, size, store
            )
            return carry

        lax.fori_loop(0, half, body, 0)
        for j in range(slab.shape[1] // LANES):
            for l in range(wide.shape[0]):
                chunk = slab[l, LANES * j : LANES * (j + 1), :]
                turned[h][0, LANES * l : LANES * (l + 1), LANES * j : LANES * (j + 1)] = (
                    chunk.T.astype(BF16)
                )


def prepare_bra(tables, beta, vectors, atoms, size, block):
    half = tables[1].shape[0] // 2
    rows, width = beta.shape[1:]
    out = jax.ShapeDtypeStruct((2, half, block, width), BF16)
    return pl.pallas_call(
        functools.partial(bra_kernel, atoms, size),
        grid=(2,),
        in_specs=[SMEM] * 5
        + [
            pl.BlockSpec((1, rows, width), lambda c: (c, 0, 0)),
            pl.BlockSpec(vectors.shape, lambda c: (0, 0)),
        ],
        out_specs=[pl.BlockSpec((1, half, block, width), lambda c: (c, 0, 0, 0))] * 4,
        out_shape=[out] * 4,
        scratch_shapes=[
            pltpu.VMEM((width // LANES, rows, LANES), F32),
            pltpu.VMEM((width // LANES, block, LANES), F32),
            pltpu.VMEM((width // LANES, block, LANES), F32),
        ],
        cost_estimate=cost(8_000_000_000, 12_000_000),
    )(*tables, beta, vectors)


def prepare_ket(tables, beta, vectors, atoms, size, block):
    half = tables[1].shape[0] // 2
    rows, width = beta.shape[1:]
    out = jax.ShapeDtypeStruct((2, width, 2 * half * block), BF16)
    return pl.pallas_call(
        functools.partial(ket_kernel, atoms, size, block),
        grid=(2,),
        in_specs=[SMEM] * 5
        + [
            pl.BlockSpec((1, rows, width), lambda c: (c, 0, 0)),
            pl.BlockSpec(vectors.shape, lambda c: (0, 0)),
        ],
        out_specs=[pl.BlockSpec((1, width, 2 * half * block), lambda c: (c, 0, 0))] * 2,
        out_shape=[out] * 2,
        scratch_shapes=[
            pltpu.VMEM((width // LANES, rows, LANES), F32),
            pltpu.VMEM((width // LANES, 2 * half * block, LANES), F32),
        ],
        cost_estimate=cost(8_000_000_000, 12_000_000),
    )(*tables, beta, vectors)


def wave_kernel(arrived_ref, place_ref, left_ref, waves_ref, out_ref):
    bands = arrived_ref.shape[1] // 2
    rows = jnp.dot(place_ref[...], arrived_ref[...], preferred_element_type=F32).astype(BF16)
    waves_ref[0] = rows
    waves_ref[1, :, :bands] = rows[:, bands:]
    waves_ref[1, :, bands:] = -rows[:, :bands]
    project_kernel(waves_ref, left_ref, out_ref)


def project_kernel(waves_ref, left_ref, out_ref):
    total = jnp.dot(left_ref[0], waves_ref[0], preferred_element_type=F32)
    total += jnp.dot(left_ref[1], waves_ref[1], preferred_element_type=F32)
    out_ref[...] = total.astype(out_ref.dtype)


def first_project(arrived, place, left):
    rows, width = arrived.shape
    return pl.pallas_call(
        wave_kernel,
        out_shape=(
            jax.ShapeDtypeStruct((2, place.shape[0], width), BF16),
            jax.ShapeDtypeStruct((left.shape[1], width), BF16),
        ),
        cost_estimate=cost(4 * left.shape[1] * rows * width, 4_000_000),
    )(arrived, place, left)


def project(waves, left, kind):
    return pl.pallas_call(
        project_kernel,
        out_shape=jax.ShapeDtypeStruct((left.shape[1], waves.shape[2]), kind),
        cost_estimate=cost(4 * left.shape[1] * waves.shape[1] * waves.shape[2], 4_000_000),
    )(waves, left)


def couple_kernel(matrix_ref, *refs):
    for kept, came, out in zip(refs[0:2], refs[2:4], refs[4:6]):
        total = kept[...] + came[...].astype(F32)
        out[...] = jnp.dot(
            matrix_ref[...],
            total,
            precision=lax.Precision.HIGHEST,
            preferred_element_type=F32,
        ).astype(BF16)


def couple(matrix, kept, came):
    out = jax.ShapeDtypeStruct(kept[0].shape, BF16)
    return pl.pallas_call(
        couple_kernel,
        out_shape=(out, out),
        cost_estimate=cost(200_000_000, 1_000_000),
    )(matrix, *kept, *came)


def back_first_kernel(left_ref, z_ref, x_ref, out_ref):
    right = jnp.concatenate([z_ref[...], x_ref[...]], axis=0)
    for part in range(2):
        out_ref[part] = jnp.dot(left_ref[part], right, preferred_element_type=F32)


def back_last_kernel(left_ref, z_ref, x_ref, start_ref, out_ref):
    right = jnp.concatenate([z_ref[...], x_ref[...]], axis=0)
    bands = out_ref.shape[2]
    real, imag = (
        start_ref[part] + jnp.dot(left_ref[part], right, preferred_element_type=F32)
        for part in range(2)
    )
    out_ref[0] = (-(real[:, bands:] + imag[:, :bands])).astype(BF16)
    out_ref[1] = (real[:, :bands] - imag[:, bands:]).astype(BF16)


def back_first(left, z, x):
    return pl.pallas_call(
        back_first_kernel,
        out_shape=jax.ShapeDtypeStruct((2, left.shape[1], z.shape[1]), F32),
        cost_estimate=cost(4 * left.shape[1] * left.shape[2] * z.shape[1], 6_000_000),
    )(left, z, x)


def back_last(left, z, x, start):
    return pl.pallas_call(
        back_last_kernel,
        out_shape=jax.ShapeDtypeStruct((2, left.shape[1], z.shape[1] // 2), BF16),
        cost_estimate=cost(4 * left.shape[1] * left.shape[2] * z.shape[1], 6_000_000),
    )(left, z, x, start)


def trade(value, bit):
    members = lax.axis_size("ga")
    return lax.ppermute(value, "ga", [(i, i ^ (1 << bit)) for i in range(members)])


def on_device(psi_k, beta_k, beta_kq, g_k, g_kq, send_index, recv_index, dmat, displaced, mode):
    groups = lax.axis_size("ga")
    count = groups.bit_length() - 1
    capacity = send_index.shape[2]
    slots = groups * capacity
    size = dmat.shape[1]
    atoms = displaced.shape[0] // groups
    block = -(-atoms * size // 8) * 8
    if block * groups % LANES:
        block = -(-block // 16) * 16
    me = lax.axis_index("ga").astype(jnp.int32)
    streams = stage_bits(count)
    orders = [block_order(bits) for bits in streams]
    swap = np.array([orders[1].index(k) for k in orders[0]], np.int32)
    tables = (
        me.reshape(1),
        jnp.asarray(np.array(orders[0], np.int32)),
        jnp.asarray(swap),
        displaced,
        mode,
    )

    packed = pack_rows(send_index.reshape(1, slots), psi_k)
    arrived = lax.all_to_all(
        packed.reshape(groups, capacity, -1), "ga", split_axis=0, concat_axis=0, tiled=True
    ).reshape(slots, -1)
    place = place_matrix(recv_index.reshape(1, -1), slots)
    lefts = prepare_bra(tables, jnp.swapaxes(beta_k, 1, 2), g_k, atoms, size, block)
    lefts = [left.reshape(2, -1, left.shape[3]) for left in lefts]

    own = lax.dynamic_slice_in_dim(displaced, me * atoms, atoms)
    coupling = jnp.take(dmat, own, axis=0)
    matrix = (jnp.eye(atoms, dtype=F32)[:, None, :, None] * coupling[:, :, None, :]).reshape(
        atoms * size, atoms * size
    )
    spare = block - atoms * size
    matrix = jnp.pad(matrix, ((0, spare), (0, spare)))

    waves, away_first = first_project(arrived, place, lefts[1])
    came_first = trade(away_first, streams[0][0])
    away_second = project(waves, lefts[3], BF16)
    came_second = trade(away_second, streams[1][0])
    kept = [project(waves, lefts[0], F32), project(waves, lefts[2], F32)]
    came = [came_first, came_second]

    for stage in range(1, count):
        away = []
        for s in range(2):
            total = (kept[s] + came[s].astype(F32)).reshape(2, -1, kept[s].shape[1])
            kept[s] = total[0]
            away.append(total[1].astype(BF16))
        came = [trade(away[s], streams[s][stage]) for s in range(2)]

    gathered = list(couple(matrix, kept, came))
    turned = prepare_ket(tables, jnp.swapaxes(beta_kq, 1, 2), g_kq, atoms, size, block)
    for stage in range(count - 1, 0, -1):
        came = [trade(gathered[s], streams[s][stage]) for s in range(2)]
        gathered = [jnp.concatenate([gathered[s], came[s]], axis=0) for s in range(2)]
    came = [trade(gathered[s], streams[s][0]) for s in range(2)]
    start = back_first(turned[0], gathered[1], gathered[0])
    return back_last(turned[1], came[1], came[0], start)


def solution(mesh):
    in_specs = (
        P(None, "ga", None),
        P(None, "ga", None),
        P(None, "ga", None),
        P(None, "ga"),
        P(None, "ga"),
        P("ga", None, None),
        P("ga"),
        P(),
        P("pert"),
        P(None, "pert"),
    )
    out_specs = P("pert", "ga", None)
    return jax.shard_map(
        on_device, mesh=mesh, in_specs=in_specs, out_specs=out_specs, check_vma=False
    )
```

```python
import functools

import jax
import jax.numpy as jnp
import numpy as np
from jax import lax
from jax.experimental import pallas as pl
from jax.experimental.pallas import tpu as pltpu
from jax.sharding import PartitionSpec as P

F32, BF16 = jnp.float32, jnp.bfloat16
LANES = 128
SMEM = pl.BlockSpec(memory_space=pltpu.SMEM)


def stage_bits(count):
    first = list(range(count))
    second = list(first)
    if count > 2:
        second[1], second[2] = 2, 1
    return first, second


def block_order(bits):
    count = len(bits)
    return [
        sum(((place >> (count - 1 - i)) & 1) << bits[i] for i in range(count))
        for place in range(1 << count)
    ]


VMEM = pltpu.VMEM
WHOLE = pl.BlockSpec(memory_space=pltpu.VMEM)
ANY = pl.BlockSpec(memory_space=pl.ANY)
MIB = 1 << 20


def call(kernel, outs, args, flops, limit, after=()):
    def body(*refs):
        kernel(*refs[len(after) :])

    body.__name__ = kernel.__name__
    moved = sum(a.size * a.dtype.itemsize for a in args)
    return pl.pallas_call(
        body,
        out_shape=[VMEM(shape, kind) for shape, kind in outs],
        in_specs=[ANY] * len(after) + [WHOLE] * len(args),
        out_specs=[WHOLE] * len(outs),
        compiler_params=pltpu.CompilerParams(vmem_limit_bytes=limit * MIB),
        cost_estimate=pl.CostEstimate(flops=flops, bytes_accessed=moved, transcendentals=0),
    )(*after, *[pltpu.with_memory_space_constraint(a, VMEM) for a in args])


def pack_kernel(send_ref, psi_ref, out_ref):
    groups, capacity = send_ref.shape
    rows, slots, bands = psi_ref.shape[1], groups * capacity, psi_ref.shape[2]
    lane = lax.broadcasted_iota(jnp.int32, (capacity, slots), 1)
    inner = lax.broadcasted_iota(jnp.int32, (capacity, slots), 0)
    spread = jnp.dot(
        send_ref[...].astype(F32),
        (lane % capacity == inner).astype(F32),
        precision=lax.Precision.HIGHEST,
        preferred_element_type=F32,
    )
    lane = lax.broadcasted_iota(jnp.int32, (groups, slots), 1)
    outer = lax.broadcasted_iota(jnp.int32, (groups, slots), 0)
    flat = jnp.sum(jnp.where(lane // capacity == outer, spread, 0.0), axis=0, keepdims=True)
    row = lax.broadcasted_iota(jnp.int32, (rows, slots), 0)
    chosen = (row == flat.astype(jnp.int32)).astype(BF16)
    for part in range(2):
        picked = lax.dot_general(
            chosen, psi_ref[part], (((0,), (0,)), ((), ())), preferred_element_type=F32
        )
        out_ref[:, part * bands : (part + 1) * bands] = picked.astype(BF16)


def pack_rows(send, psi):
    count = send.shape[0] * send.shape[1]
    return pl.pallas_call(
        pack_kernel,
        out_shape=jax.ShapeDtypeStruct((count, 2 * psi.shape[2]), BF16),
        compiler_params=pltpu.CompilerParams(vmem_limit_bytes=12 * MIB),
        cost_estimate=pl.CostEstimate(
            flops=300_000_000, bytes_accessed=1_000_000, transcendentals=0
        ),
    )(send, psi)


def place_kernel(recv_ref, out_ref):
    chosen = lax.broadcasted_iota(jnp.int32, out_ref.shape, 0) == recv_ref[...]
    out_ref[...] = chosen.astype(F32).T.astype(BF16)


def place_matrix(recv, slots):
    return call(place_kernel, [((recv.shape[1], slots), BF16)], [recv], 1_000_000_000, 8)[0]


def widen_rows(source, part, wide):
    rows, step = source.shape[1], 96
    while rows % step:
        step -= 8

    def body(index, carry):
        start = pl.multiple_of(index * step, 8)
        for l in range(wide.shape[0]):
            lanes = slice(LANES * l, LANES * (l + 1))
            wide[l, pl.ds(start, step), :] = source[part, pl.ds(start, step), lanes].astype(F32)
        return carry

    lax.fori_loop(0, rows // step, body, 0)


def walk_atoms(wide, tables, vectors, place, atoms, size, store):
    home, order, displaced, mode = tables
    base = (home[0] ^ order[place]) * atoms
    for i in range(atoms):
        start = displaced[base + i] * size
        amount = [mode[x, base + i] for x in range(3)]
        for l in range(wide.shape[0]):
            lanes = slice(LANES * l, LANES * (l + 1))
            picked = wide[l, pl.ds(start, size), :]
            weight = (
                amount[0] * vectors[0:1, lanes]
                + amount[1] * vectors[1:2, lanes]
                + amount[2] * vectors[2:3, lanes]
            )
            store(i, l, picked, weight)


def bra_kernel(atoms, size, tables, source, vectors, plain, scaled, wide, slabs, finished):
    half, block = plain[0].shape[1:3]
    swap = tables[1]
    tables = (tables[0], *tables[2:])
    slab, slab_scaled = slabs
    if block != atoms * size:
        slab[...] = jnp.zeros_like(slab)
        slab_scaled[...] = jnp.zeros_like(slab_scaled)

    def store(i, l, picked, weight):
        slab[l, size * i : size * (i + 1), :] = picked
        slab_scaled[l, size * i : size * (i + 1), :] = picked * weight

    for part in range(2):
        widen_rows(source, part, wide)
        for h in range(2):

            def body(index, carry):
                place = h * half + index
                walk_atoms(wide, tables, vectors, place, atoms, size, store)
                other = swap[place] - h * half
                for l in range(wide.shape[0]):
                    lanes = slice(LANES * l, LANES * (l + 1))
                    plain[h][part, index, :, lanes] = slab[l].astype(BF16)
                    scaled[h][part, other, :, lanes] = slab_scaled[l].astype(BF16)
                return carry

            lax.fori_loop(0, half, body, 0)
        finished(part)


def ket_kernel(atoms, size, block, tables, source, vectors, turned, wide, slab):
    half = slab.shape[1] // (2 * block)
    swap = tables[1]
    tables = (tables[0], *tables[2:])
    if block != atoms * size:
        slab[...] = jnp.zeros_like(slab)
    for part in range(2):
        widen_rows(source, part, wide)
        for h in range(2):

            def body(index, carry):
                place = h * half + index
                plain_row = pl.multiple_of((swap[place] - h * half) * block, 8)
                scaled_row = pl.multiple_of((half + index) * block, 8)

                def store(i, l, picked, weight):
                    slab[l, pl.ds(plain_row + size * i, size), :] = picked
                    slab[l, pl.ds(scaled_row + size * i, size), :] = -(picked * weight)

                walk_atoms(wide, tables, vectors, place, atoms, size, store)
                return carry

            lax.fori_loop(0, half, body, 0)
            for j in range(slab.shape[1] // LANES):
                columns = slice(LANES * j, LANES * (j + 1))
                for l in range(wide.shape[0]):
                    lanes = slice(LANES * l, LANES * (l + 1))
                    turned[h][part, lanes, columns] = slab[l, columns, :].T.astype(BF16)


def prepare_bra(tables, beta, vectors, atoms, size, block, after):
    half = tables[1].shape[0] // 2
    rows, width = beta.shape[1:]
    tiles = width // LANES
    skip = len(after)
    shape = (2, half, block, width)

    def body(*refs):
        home, swap, order, displaced, mode, source, vectors_ref = refs[skip : skip + 7]
        ready, outs = refs[skip + 7], refs[skip + 8 : skip + 11]
        staged, sent, scratch = refs[skip + 11 : skip + 14], refs[skip + 14], refs[skip + 15 :]
        copies = [
            [
                pltpu.make_async_copy(staged[n].at[part], outs[n].at[part], sent.at[n, part])
                for n in range(3)
            ]
            for part in range(2)
        ]

        def finished(part):
            for copy in copies[part]:
                copy.start()

        bra_kernel(
            atoms, size, (home, swap, order, displaced, mode), source, vectors_ref,
            (staged[0], ready), (staged[1], staged[2]), scratch[0], scratch[1:3], finished,
        )
        for group in copies:
            for copy in group:
                copy.wait()

    ready, *rest = pl.pallas_call(
        body,
        in_specs=[ANY] * skip + [SMEM] * 5 + [WHOLE, WHOLE],
        out_specs=[WHOLE] + [pl.BlockSpec(memory_space=pltpu.HBM)] * 3,
        out_shape=[VMEM(shape, BF16)] + [pltpu.HBM(shape, BF16)] * 3,
        scratch_shapes=[VMEM(shape, BF16)] * 3
        + [
            pltpu.SemaphoreType.DMA((3, 2)),
            VMEM((tiles, rows, LANES), F32),
            VMEM((tiles, block, LANES), F32),
            VMEM((tiles, block, LANES), F32),
        ],
        compiler_params=pltpu.CompilerParams(vmem_limit_bytes=14 * MIB),
        cost_estimate=pl.CostEstimate(
            flops=8_000_000_000, bytes_accessed=12_000_000, transcendentals=0
        ),
    )(*after, *tables, pltpu.with_memory_space_constraint(beta, VMEM), vectors)
    return rest[0], ready, rest[1], rest[2]


def prepare_ket(tables, beta, vectors, atoms, size, block, after):
    half = tables[1].shape[0] // 2
    rows, width = beta.shape[1:]
    tiles, depth = width // LANES, 2 * half * block
    skip = len(after)

    def body(*refs):
        home, swap, order, displaced, mode, source, vectors_ref = refs[skip : skip + 7]
        outs, token, scratch = refs[skip + 7 : skip + 9], refs[skip + 9], refs[skip + 10 :]
        ket_kernel(
            atoms, size, block, (home, swap, order, displaced, mode), source, vectors_ref,
            outs, *scratch,
        )
        token[...] = jnp.zeros_like(token)

    return pl.pallas_call(
        body,
        in_specs=[ANY] * skip + [SMEM] * 5 + [WHOLE, WHOLE],
        out_specs=[WHOLE] * 3,
        out_shape=[VMEM((2, width, depth), BF16)] * 2 + [VMEM((8, LANES), F32)],
        scratch_shapes=[
            VMEM((tiles, rows, LANES), F32),
            VMEM((tiles, depth, LANES), F32),
        ],
        compiler_params=pltpu.CompilerParams(vmem_limit_bytes=14 * MIB),
        cost_estimate=pl.CostEstimate(
            flops=8_000_000_000, bytes_accessed=12_000_000, transcendentals=0
        ),
    )(*after, *tables, pltpu.with_memory_space_constraint(beta, VMEM), vectors)


def project_kernel(waves_ref, left_ref, out_ref):
    total = jnp.dot(left_ref[0], waves_ref[0], preferred_element_type=F32)
    total += jnp.dot(left_ref[1], waves_ref[1], preferred_element_type=F32)
    out_ref[...] = total.astype(out_ref.dtype)


def wave_kernel(arrived_ref, place_ref, left_ref, waves_ref, out_ref):
    bands = arrived_ref.shape[1] // 2
    rows = jnp.dot(place_ref[...], arrived_ref[...], preferred_element_type=F32).astype(BF16)
    waves_ref[0] = rows
    waves_ref[1, :, :bands] = rows[:, bands:]
    waves_ref[1, :, bands:] = -rows[:, :bands]
    project_kernel(waves_ref, left_ref, out_ref)


def first_project(arrived, place, left):
    width = arrived.shape[1]
    outs = [((2, place.shape[0], width), BF16), ((left.shape[1], width), BF16)]
    return call(wave_kernel, outs, [arrived, place, left], 1_200_000_000, 14)


def project(waves, left, kind, after=()):
    outs = [((left.shape[1], waves.shape[2]), kind)]
    return call(project_kernel, outs, [waves, left], 900_000_000, 14, after)[0]


def fold_kernel(kept_ref, came_ref, next_ref, away_ref):
    rows = next_ref.shape[0]
    next_ref[...] = kept_ref[:rows] + came_ref[:rows].astype(F32)
    away_ref[...] = (kept_ref[rows:] + came_ref[rows:].astype(F32)).astype(BF16)


def fold(kept, came, after=()):
    rows, width = kept.shape[0] // 2, kept.shape[1]
    outs = [((rows, width), F32), ((rows, width), BF16)]
    return call(fold_kernel, outs, [kept, came], 1_000_000, 4, after)


def couple_kernel(matrix_ref, *refs):
    for kept, came, out in zip(refs[0:2], refs[2:4], refs[4:6]):
        out[...] = jnp.dot(
            matrix_ref[...],
            kept[...] + came[...].astype(F32),
            precision=lax.Precision.HIGHEST,
            preferred_element_type=F32,
        ).astype(BF16)


def couple(matrix, kept, came):
    outs = [(kept[0].shape, BF16)] * 2
    return call(couple_kernel, outs, [matrix, *kept, *came], 200_000_000, 6)


def join_kernel(own_ref, came_ref, out_ref):
    rows = own_ref.shape[0]
    out_ref[:rows] = own_ref[...]
    out_ref[rows:] = came_ref[...]


def join(own, came):
    outs = [((2 * own.shape[0], own.shape[1]), BF16)]
    return call(join_kernel, outs, [own, came], 1_000_000, 4)[0]


def back_kernel(low, high, start, left_ref, *refs):
    out_ref = refs[-1]
    right = jnp.concatenate([ref[...] for ref in refs[: len(refs) - 1 - start]], axis=0)
    right = right[: high - low]
    total = []
    for part in range(2):
        product = jnp.dot(left_ref[part, :, low:high], right, preferred_element_type=F32)
        total.append(refs[-2][part] + product if start else product)
    if out_ref.dtype == F32:
        out_ref[0], out_ref[1] = total
    else:
        bands = out_ref.shape[2]
        real, imag = total
        out_ref[0] = (-(real[:, bands:] + imag[:, :bands])).astype(BF16)
        out_ref[1] = (real[:, :bands] - imag[:, bands:]).astype(BF16)


def back_partial(left, low, high, rights, start=()):
    kernel = functools.partial(back_kernel, low, high, len(start))
    kernel.__name__ = "back_kernel"
    outs = [((2, left.shape[1], rights[0].shape[1]), F32)]
    flops = 4 * left.shape[1] * (high - low) * rights[0].shape[1]
    return call(kernel, outs, [left, *rights, *start], flops, 20)[0]


def back_last(left, high, rights, start):
    args = [left, *rights, start]
    return pl.pallas_call(
        functools.partial(back_kernel, 0, high, 1),
        in_specs=[WHOLE] * len(args),
        out_specs=WHOLE,
        out_shape=jax.ShapeDtypeStruct((2, left.shape[1], rights[0].shape[1] // 2), BF16),
        compiler_params=pltpu.CompilerParams(vmem_limit_bytes=20 * MIB),
        cost_estimate=pl.CostEstimate(
            flops=2_000_000_000, bytes_accessed=6_000_000, transcendentals=0
        ),
    )(*[pltpu.with_memory_space_constraint(a, VMEM) for a in args])


def trade(value, bit):
    members = lax.axis_size("ga")
    return lax.ppermute(value, "ga", [(i, i ^ (1 << bit)) for i in range(members)])


def on_device(psi_k, beta_k, beta_kq, g_k, g_kq, send_index, recv_index, dmat, displaced, mode):
    groups = lax.axis_size("ga")
    count = groups.bit_length() - 1
    capacity = send_index.shape[2]
    slots = groups * capacity
    size = dmat.shape[1]
    atoms = displaced.shape[0] // groups
    block = -(-atoms * size // 8) * 8
    if block * groups % LANES:
        block = -(-block // 16) * 16
    me = lax.axis_index("ga").astype(jnp.int32)
    streams = stage_bits(count)
    orders = [block_order(bits) for bits in streams]
    swap = np.array([orders[1].index(k) for k in orders[0]], np.int32)
    tables = (
        me.reshape(1),
        jnp.asarray(swap),
        jnp.asarray(np.array(orders[0], np.int32)),
        displaced,
        mode,
    )

    packed = pack_rows(send_index[0], psi_k)
    arrived = lax.all_to_all(
        packed.reshape(groups, capacity, -1), "ga", split_axis=0, concat_axis=0, tiled=True
    ).reshape(slots, -1)

    own = lax.dynamic_slice_in_dim(displaced, me * atoms, atoms)
    coupling = jnp.take(dmat, own, axis=0)
    matrix = (jnp.eye(atoms, dtype=F32)[:, None, :, None] * coupling[:, :, None, :]).reshape(
        atoms * size, atoms * size
    )
    spare = block - atoms * size
    matrix = jnp.pad(matrix, ((0, spare), (0, spare)))
    place = place_matrix(recv_index.reshape(1, -1), slots)
    lefts = prepare_bra(
        tables, jnp.swapaxes(beta_k, 1, 2), g_k, atoms, size, block, (matrix[:1, :1],)
    )
    lefts = [left.reshape(2, -1, left.shape[3]) for left in lefts]

    waves, away_first = first_project(arrived, place, lefts[1])
    came_first = trade(away_first, streams[0][0])
    away_second = project(waves, lefts[3], BF16)
    came_second = trade(away_second, streams[1][0])
    kept = [project(waves, lefts[0], F32), project(waves, lefts[2], F32)]
    came = [came_first, came_second]
    token = ()
    for stage in range(1, count):
        away = [None, None]
        for s in range(2):
            behind = () if s == 0 else (away[0][:8, :LANES],)
            kept[s], away[s] = fold(kept[s], came[s], (*token, *behind))
        came = [trade(away[s], streams[s][stage]) for s in range(2)]
        if stage == 1:
            *turned, token = prepare_ket(
                tables, jnp.swapaxes(beta_kq, 1, 2), g_kq, atoms, size, block,
                (away[0][:8, :LANES], away[1][:8, :LANES]),
            )
            token = (token,)
        else:
            token = ()

    gathered = list(couple(matrix, kept, came))
    for stage in range(count - 1, 0, -1):
        came = [trade(gathered[s], streams[s][stage]) for s in range(2)]
        gathered = [join(gathered[s], came[s]) for s in range(2)]
    came = [trade(gathered[s], streams[s][0]) for s in range(2)]
    rows = gathered[0].shape[0]
    start = back_partial(turned[0], 0, 2 * rows, [gathered[1], gathered[0]])
    cut = -(-rows // LANES) * LANES
    start = back_partial(turned[1], cut, 2 * rows, [came[0][cut - rows :]], [start])
    return back_last(turned[1], cut, [came[1], came[0][: max(cut - rows, 8)]], start)


def solution(mesh):
    in_specs = (
        P(None, "ga", None),
        P(None, "ga", None),
        P(None, "ga", None),
        P(None, "ga"),
        P(None, "ga"),
        P("ga", None, None),
        P("ga"),
        P(),
        P("pert"),
        P(None, "pert"),
    )
    out_specs = P("pert", "ga", None)
    return jax.shard_map(
        on_device, mesh=mesh, in_specs=in_specs, out_specs=out_specs, check_vma=False
    )
```
